256 devices in a mesh: blk: 128 (over z, x, y), rep: 2 (over core).
Axes of the slice: x: 4, y: 4, z: 8, core: 2. Of those that a mesh axis runs over, the one named last changes fastest.
Arguments:
- points: float32 [128, 3, 8192], P('blk'), may hold values from -6 to 6
- normals: float32 [128, 3, 8192], P('blk'), may hold values from -6 to 6
- src_block: int32 [8, 128, 1, 16], P(None, 'blk', None, 'rep'), may hold values from 0 to 63
- tgt_index: int32 [8, 128, 1, 16, 128], P(None, 'blk', None, 'rep'), may hold values from 0 to 8191
- active: int32 [8, 128, 1], P(None, 'blk'), may hold values from 0 to 16
Outputs:
- diag_hess: float32 [128, 36], P('blk')
- gradient: float32 [128, 6], P('blk')
- pair_hess: float32 [8, 128, 1, 36], P(None, 'blk')
The draws below stay inside these ranges and needn't reach their ends.
Inputs may be any that keep to these rules, and one draw needn't show every extreme that they name: Slots j with j >= active contribute nothing.
All inputs are finite; a program needn't handle non-finite values.
Results may differ from the reference program's by a relative error of at most 0.00017.
Values sent between devices are 32-bit elements; how exact they have to be, the bound alone decides.
A program may use at most 64 MiB of HBM per device.

```python
import jax
import jax.numpy as jnp
from jax import lax

SC = 1
P_SIZE = 8192
NB = 16
BLOCK = 128
ROUNDS = 8
NSCANS = 128
N_BLK = 128


def place_ends(values, key, low, high):
    longest = values.shape.index(max(values.shape))
    spots = []
    for shift in (0, 1):
        where = [jax.random.randint(jax.random.fold_in(key, axis), (), 0, length) for axis, length in enumerate(values.shape)]
        where[longest] = (where[longest] + shift) % values.shape[longest]
        spots.append(tuple(where))
    return values.at[spots[0]].set(low).at[spots[1]].set(high)


def level_of(rng, extent, shards, low, high):
    level = 1.0
    for dim, shards_of in shards:
        steps = jax.random.uniform(jax.random.fold_in(jax.random.fold_in(rng, 6), dim), (shards_of,), jnp.float32, low / len(shards), high / len(shards))
        level = level * jnp.repeat(jnp.exp(steps), extent[dim] // shards_of).reshape((-1,) + (1,) * (len(extent) - 1 - dim))
    return level


def gaussian(key, extent, width, limit, pieces=(), kind=jnp.bfloat16):
    gain = level_of(key, extent, pieces, -0.22, 0.18) if pieces else 1.0
    drawn = jax.random.normal(key, extent, jnp.float32) * width * gain
    return jnp.minimum(jnp.maximum(drawn, -limit), limit).astype(kind)


def setup_inputs(seed: int = 0) -> dict:
    key_of = jax.random.split(jax.random.key(seed), 6)
    return {
        "points": gaussian(key_of[0], (NSCANS, 3, P_SIZE), 0.5, 6.0, ((0, 128),), jnp.float32),
        "normals": gaussian(key_of[1], (NSCANS, 3, P_SIZE), 1.0, 6.0, ((0, 128),), jnp.float32),
        "src_block": place_ends(jax.random.randint(key_of[2], (ROUNDS, NSCANS, SC, NB), 0, P_SIZE // BLOCK), jax.random.fold_in(key_of[2], 1), 0, (P_SIZE // BLOCK) - 1).astype(jnp.int32),
        "tgt_index": place_ends(jax.random.randint(key_of[3], (ROUNDS, NSCANS, SC, NB, BLOCK), 0, P_SIZE), jax.random.fold_in(key_of[3], 1), 0, P_SIZE - 1).astype(jnp.int32),
        "active": place_ends(jax.random.randint(key_of[4], (ROUNDS, NSCANS, SC), 0, NB + 1), jax.random.fold_in(key_of[4], 1), 0, NB).astype(jnp.int32),
    }


def reference(points, normals, src_block, tgt_index, active):
    nscans = points.shape[0]
    npts = points.shape[2]
    slots = NB * BLOCK
    flat_p = jnp.moveaxis(points, 1, 0).reshape(3, -1)
    flat_n = jnp.moveaxis(normals, 1, 0).reshape(3, -1)
    lanes = jnp.arange(BLOCK, dtype=jnp.int32)
    owner = jnp.arange(nscans, dtype=jnp.int32) // SC
    local = jnp.arange(SC, dtype=jnp.int32)
    scans = jnp.arange(nscans, dtype=jnp.int32)
    slot_block = jnp.arange(slots, dtype=jnp.int32) // BLOCK
    diag = jnp.zeros((nscans, 36), jnp.float32)
    grad = jnp.zeros((nscans, 6), jnp.float32)
    pairs = []
    for k in range(1, ROUNDS + 1):
        tscan = (((owner[:, None] - k) % N_BLK) * SC + local[None, :]).astype(jnp.int32)
        sidx = (scans[:, None, None, None] * npts + src_block[k - 1][:, :, :, None] * BLOCK + lanes).reshape(nscans, SC, slots)
        tidx = tscan[:, :, None] * npts + tgt_index[k - 1].reshape(nscans, SC, slots)
        p = flat_p[:, sidx]
        q = flat_p[:, tidx]
        n = flat_n[:, tidx]
        live = (slot_block[None, None, :] < active[k - 1][:, :, None]).astype(jnp.float32)
        resid = jnp.sum(n * (p - q), axis=0)
        weight = live / (1.0 + resid * resid)
        jacob = jnp.stack([p[1] * n[2] - p[2] * n[1], p[2] * n[0] - p[0] * n[2], p[0] * n[1] - p[1] * n[0], n[0], n[1], n[2]])
        gram = jnp.einsum('iast,jast->asij', jacob * weight, jacob, precision=lax.Precision.HIGHEST) / (NB * BLOCK)
        push = jnp.einsum('iast,ast->asi', jacob, weight * resid, precision=lax.Precision.HIGHEST) / (NB * BLOCK)
        gram = gram.reshape(nscans, SC, 36)
        pairs.append(gram)
        diag = diag + gram.sum(1)
        grad = grad + push.sum(1)
        diag = diag.at[tscan.reshape(-1)].add(gram.reshape(-1, 36))
        grad = grad.at[tscan.reshape(-1)].add(-push.reshape(-1, 6))
    scale = 2.0 * ROUNDS * SC
    return diag / scale, grad / scale, jnp.stack(pairs)
```

```python
import functools

import jax
import jax.numpy as jnp
from jax import lax
from jax.experimental import pallas as pl
from jax.experimental.pallas import tpu as pltpu
from jax.sharding import PartitionSpec as P

MESH = pl.DeviceIdType.MESH
LANES = 128
ENTRIES = [(i, j) for i in range(6) for j in range(i, 6)]


def kernel(
    n_blk, rounds, nslots, npts, total_slots,
    pts_hbm, nrm_hbm, src_hbm, tgt_hbm, act_hbm,
    diag_ref, grad_ref, pair_ref,
    pts, nrm, tgt, src, act,
    p_send, a_send, i_recv, p_recv, a_recv,
    prods, r_send, r_recv, t_send, t_recv,
    local_sem, i_ssem, i_rsem, p_ssem, p_rsem, a_ssem, a_rsem,
    r_ssem, r_rsem, t_ssem, t_rsem,
):
    me = lax.axis_index("blk")
    rep = lax.axis_index("rep")
    rows = npts // LANES

    def up(k):
        return lax.rem(me + k, n_blk)

    def down(k):
        return lax.rem(me + n_blk - k, n_blk)

    barrier = pltpu.get_barrier_semaphore()
    for k in range(1, rounds + 1):
        pl.semaphore_signal(barrier, inc=1, device_id=(up(k), rep), device_id_type=MESH)
        for half in range(2):
            pl.semaphore_signal(barrier, inc=1, device_id=(down(k), half), device_id_type=MESH)
    pl.semaphore_signal(barrier, inc=1, device_id=(me, 1 - rep), device_id_type=MESH)

    loads = [
        pltpu.make_async_copy(src_hbm, src, local_sem.at[0]),
        pltpu.make_async_copy(act_hbm, act, local_sem.at[1]),
        pltpu.make_async_copy(pts_hbm, pts, local_sem.at[2]),
        pltpu.make_async_copy(tgt_hbm, tgt, local_sem.at[3]),
        pltpu.make_async_copy(nrm_hbm, nrm, local_sem.at[4]),
    ]
    for load in loads:
        load.start()
    for load in loads:
        load.wait()

    for k in range(rounds):
        for j in range(nslots):
            block = src[k, j]
            for c in range(3):
                p_send[k, c, pl.ds(j, 1), :] = pts[c, pl.ds(block, 1), :]
        a_send[k] = jnp.full((1, LANES), act[0, k], jnp.int32)

    pl.semaphore_wait(barrier, 3 * rounds + 1)

    sends = []
    order = list(range(rounds))
    for k in reversed(order):
        to = (down(k + 1), rep)
        for source, target, ssem, rsem in (
            (tgt.at[k], i_recv.at[k], i_ssem.at[k], i_rsem.at[k]),
            (a_send.at[k], a_recv.at[k], a_ssem.at[k], a_rsem.at[k]),
            (p_send.at[k], p_recv.at[k], p_ssem.at[k], p_rsem.at[k]),
        ):
            copy = pltpu.make_async_remote_copy(
                src_ref=source, dst_ref=target, send_sem=ssem, recv_sem=rsem,
                device_id=to, device_id_type=MESH,
            )
            copy.start()
            sends.append((k, copy))

    sub = lax.broadcasted_iota(jnp.int32, (nslots, LANES), 0)
    lane = lax.broadcasted_iota(jnp.int32, (nslots, LANES), 1)
    slot_of = sub + rep * nslots
    li, lj = lane // 6, lane % 6
    lo, hi = jnp.minimum(li, lj), jnp.maximum(li, lj)
    entry_of = jnp.where(
        lane < 36, lo * 6 - (lo * (lo - 1)) // 2 + hi - lo,
        jnp.where(lane < 42, lane - 36 + 21, -1),
    )

    tsum = jnp.zeros((1, LANES), jnp.float32)
    results = []
    for k in order:
        inbound = [copy for kk, copy in sends if kk == k]
        inbound[0].wait_recv()
        index = i_recv[k]
        row_of = index // LANES
        lane_of = index % LANES

        def gather_rows(g, acc):
            acc = list(acc)
            base = pl.multiple_of(g * 8, 8)
            for table, first in ((pts, 0), (nrm, 3)):
                for c in range(3):
                    tile = table[c, pl.ds(base, 8), :]
                    for j in range(8):
                        row = jnp.broadcast_to(tile[j : j + 1], (nslots, LANES))
                        got = jnp.take_along_axis(row, lane_of, axis=1, mode="promise_in_bounds")
                        acc[first + c] = jnp.where(row_of == base + j, got, acc[first + c])
            return tuple(acc)

        zero = jnp.zeros((nslots, LANES), jnp.float32)
        q0, q1, q2, n0, n1, n2 = lax.fori_loop(0, rows // 8, gather_rows, (zero,) * 6)

        inbound[1].wait_recv()
        inbound[2].wait_recv()
        live = (slot_of < a_recv[k]).astype(jnp.float32)
        p0, p1, p2 = p_recv[k, 0], p_recv[k, 1], p_recv[k, 2]
        resid = n0 * (p0 - q0) + n1 * (p1 - q1) + n2 * (p2 - q2)
        weight = live / (1.0 + resid * resid)
        jacob = [p1 * n2 - p2 * n1, p2 * n0 - p0 * n2, p0 * n1 - p1 * n0, n0, n1, n2]
        scaled = [weight * entry for entry in jacob]
        for e, (i, j) in enumerate(ENTRIES):
            prods[pl.ds(e * 8, 8), :] = scaled[i] * jacob[j]
        for i in range(6):
            prods[pl.ds((21 + i) * 8, 8), :] = scaled[i] * resid
        spread = jnp.zeros((8, LANES), jnp.float32)
        for g in range(4):
            some = prods[pl.ds(g * 64, 8, stride=8), :]
            for t in range(1, 8):
                some = some + prods[pl.ds(g * 64 + t, 8, stride=8), :]
            whole = jnp.sum(some, axis=1, keepdims=True)
            spread = spread + jnp.where(entry_of == sub + g * 8, whole, 0.0)
        line = jnp.sum(spread, axis=0, keepdims=True)
        tsum = tsum + line
        r_send[k] = line
        for half in range(2):
            copy = pltpu.make_async_remote_copy(
                src_ref=r_send.at[k], dst_ref=r_recv.at[rep, k],
                send_sem=r_ssem.at[half, k], recv_sem=r_rsem.at[rep, k],
                device_id=(up(k + 1), half), device_id_type=MESH,
            )
            copy.start()
            results.append(copy)

    t_send[...] = tsum
    exchange = pltpu.make_async_remote_copy(
        src_ref=t_send, dst_ref=t_recv, send_sem=t_ssem, recv_sem=t_rsem,
        device_id=(me, 1 - rep), device_id_type=MESH,
    )
    exchange.start()

    lane1 = lax.broadcasted_iota(jnp.int32, (1, LANES), 1)
    source_sum = jnp.zeros((1, LANES), jnp.float32)
    for k in order:
        for half in range(2):
            pltpu.make_async_remote_copy(
                src_ref=r_send.at[k], dst_ref=r_recv.at[half, k],
                send_sem=r_ssem.at[half, k], recv_sem=r_rsem.at[half, k],
                device_id=(up(k + 1), half), device_id_type=MESH,
            ).wait_recv()
        both = (r_recv[0, k] + r_recv[1, k]) * (1.0 / total_slots)
        pair_ref[pl.ds(k, 1), :] = both[:, :36]
        source_sum = source_sum + both
    exchange.wait_recv()
    target_sum = (t_send[...] + t_recv[...]) * (1.0 / total_slots)
    final = (source_sum + jnp.where(lane1 < 36, target_sum, -target_sum)) * (1.0 / (2.0 * rounds))
    diag_ref[...] = final[:, :36]
    grad_ref[...] = final[:, 36:42]

    for _, copy in sends:
        copy.wait_send()
    for copy in results:
        copy.wait_send()
    exchange.wait_send()


def solution(mesh):
    n_blk = mesh.shape["blk"]

    def body(points, normals, src_block, tgt_index, active):
        npts = points.shape[2]
        rounds, nslots = src_block.shape[0], src_block.shape[3]
        rows = npts // LANES
        f32, i32 = jnp.float32, jnp.int32
        dma = pltpu.SemaphoreType.DMA
        diag, grad, pair = pl.pallas_call(
            functools.partial(kernel, n_blk, rounds, nslots, npts, 2 * nslots * LANES),
            out_shape=(
                jax.ShapeDtypeStruct((1, 36), f32),
                jax.ShapeDtypeStruct((1, 6), f32),
                jax.ShapeDtypeStruct((rounds, 36), f32),
            ),
            in_specs=[pl.BlockSpec(memory_space=pl.ANY)] * 5,
            out_specs=(pl.BlockSpec(memory_space=pltpu.VMEM),) * 3,
            scratch_shapes=[
                pltpu.VMEM((3, rows, LANES), f32),
                pltpu.VMEM((3, rows, LANES), f32),
                pltpu.VMEM((rounds, nslots, LANES), i32),
                pltpu.SMEM((rounds, nslots), i32),
                pltpu.SMEM((1, rounds), i32),
                pltpu.VMEM((rounds, 3, nslots, LANES), f32),
                pltpu.VMEM((rounds, 1, LANES), i32),
                pltpu.VMEM((rounds, nslots, LANES), i32),
                pltpu.VMEM((rounds, 3, nslots, LANES), f32),
                pltpu.VMEM((rounds, 1, LANES), i32),
                pltpu.VMEM((256, LANES), f32),
                pltpu.VMEM((rounds, 1, LANES), f32),
                pltpu.VMEM((2, rounds, 1, LANES), f32),
                pltpu.VMEM((1, LANES), f32),
                pltpu.VMEM((1, LANES), f32),
                dma((5,)),
                dma((rounds,)), dma((rounds,)),
                dma((rounds,)), dma((rounds,)),
                dma((rounds,)), dma((rounds,)),
                dma((2, rounds)), dma((2, rounds)),
                dma, dma,
            ],
            compiler_params=pltpu.CompilerParams(collective_id=0, has_side_effects=True),
        )(
            points.reshape(3, rows, LANES),
            normals.reshape(3, rows, LANES),
            src_block.reshape(rounds, nslots),
            tgt_index.reshape(rounds, nslots, LANES),
            active.reshape(1, rounds),
        )
        return diag, grad, pair.reshape(rounds, 1, 1, 36)

    return jax.shard_map(
        body,
        mesh=mesh,
        in_specs=(
            P("blk", None, None),
            P("blk", None, None),
            P(None, "blk", None, "rep"),
            P(None, "blk", None, "rep", None),
            P(None, "blk", None),
        ),
        out_specs=(P("blk", None), P("blk", None), P(None, "blk", None, None)),
        check_vma=False,
    )
```

```python
import functools

import jax
import jax.numpy as jnp
from jax import lax
from jax.experimental import pallas as pl
from jax.experimental.pallas import tpu as pltpu
from jax.sharding import PartitionSpec as P

MESH = pl.DeviceIdType.MESH
LANES = 128
ENTRIES = [(i, j) for i in range(6) for j in range(i, 6)]


def kernel(
    n_blk, rounds, nslots, npts,
    pts_hbm, nrm_hbm, src_hbm, tgt_hbm, act_hbm,
    out_ref,
    pts, nrm, tgt, src, act,
    p_send, a_send, i_recv, p_recv, a_recv,
    prods, r_send, r_recv, t_send, t_recv,
    local_sem, i_ssem, i_rsem, p_ssem, p_rsem, a_ssem, a_rsem,
    r_ssem, r_rsem, t_ssem, t_rsem,
):
    me = lax.axis_index("blk")
    rep = lax.axis_index("rep")
    rows = npts // LANES

    def up(k):
        return lax.rem(me + k, n_blk)

    def down(k):
        return lax.rem(me + n_blk - k, n_blk)

    barrier = pltpu.get_barrier_semaphore()
    for k in range(1, rounds + 1):
        pl.semaphore_signal(barrier, inc=1, device_id=(up(k), rep), device_id_type=MESH)
        for half in range(2):
            pl.semaphore_signal(barrier, inc=1, device_id=(down(k), half), device_id_type=MESH)
    pl.semaphore_signal(barrier, inc=1, device_id=(me, 1 - rep), device_id_type=MESH)

    loads = [
        pltpu.make_async_copy(src_hbm, src, local_sem.at[0]),
        pltpu.make_async_copy(act_hbm, act, local_sem.at[1]),
        pltpu.make_async_copy(pts_hbm, pts, local_sem.at[2]),
        pltpu.make_async_copy(tgt_hbm, tgt, local_sem.at[3]),
        pltpu.make_async_copy(nrm_hbm, nrm, local_sem.at[4]),
    ]
    for load in loads:
        load.start()
    for load in loads:
        load.wait()

    for k in range(rounds):
        for j in range(nslots):
            block = src[k, j]
            for c in range(3):
                p_send[k, c, pl.ds(j, 1), :] = pts[c, pl.ds(block, 1), :]
        a_send[k] = jnp.full((1, LANES), act[0, k], jnp.int32)

    pl.semaphore_wait(barrier, 3 * rounds + 1)

    sends = []
    order = list(range(rounds))
    for k in reversed(order):
        to = (down(k + 1), rep)
        for source, target, ssem, rsem in (
            (tgt.at[k], i_recv.at[k], i_ssem.at[k], i_rsem.at[k]),
            (a_send.at[k], a_recv.at[k], a_ssem.at[k], a_rsem.at[k]),
            (p_send.at[k], p_recv.at[k], p_ssem.at[k], p_rsem.at[k]),
        ):
            copy = pltpu.make_async_remote_copy(
                src_ref=source, dst_ref=target, send_sem=ssem, recv_sem=rsem,
                device_id=to, device_id_type=MESH,
            )
            copy.start()
            sends.append((k, copy))

    sub = lax.broadcasted_iota(jnp.int32, (nslots, LANES), 0)
    lane = lax.broadcasted_iota(jnp.int32, (nslots, LANES), 1)
    slot_of = sub + rep * nslots
    li, lj = lane // 6, lane % 6
    lo, hi = jnp.minimum(li, lj), jnp.maximum(li, lj)
    entry_of = jnp.where(
        lane < 36, lo * 6 - (lo * (lo - 1)) // 2 + hi - lo,
        jnp.where(lane < 42, lane - 36 + 21, -1),
    )

    def inbound(k, source, target, ssem, rsem):
        return pltpu.make_async_remote_copy(
            src_ref=source.at[k], dst_ref=target.at[k], send_sem=ssem.at[k], recv_sem=rsem.at[k],
            device_id=(down(k + 1), rep), device_id_type=MESH,
        )

    def returned(k, half):
        return pltpu.make_async_remote_copy(
            src_ref=r_send.at[k], dst_ref=r_recv.at[rep, k],
            send_sem=r_ssem.at[half, k], recv_sem=r_rsem.at[rep, k],
            device_id=(up(k + 1), half), device_id_type=MESH,
        )

    def one_pair(step, tsum):
        k = rounds - 1 - step
        inbound(k, tgt, i_recv, i_ssem, i_rsem).wait_recv()
        index = i_recv[k]
        row_of = lax.shift_right_logical(index, 7)
        lane_of = lax.bitwise_and(index, LANES - 1)
        acc = [jnp.zeros((nslots, LANES), jnp.float32)] * 6
        for row in range(rows):
            here = row_of == row
            for e, (table, c) in enumerate(((pts, 0), (pts, 1), (pts, 2), (nrm, 0), (nrm, 1), (nrm, 2))):
                line = jnp.broadcast_to(table[c, row : row + 1, :], (nslots, LANES))
                got = jnp.take_along_axis(line, lane_of, axis=1, mode="promise_in_bounds")
                acc[e] = jnp.where(here, got, acc[e])
        q0, q1, q2, n0, n1, n2 = acc

        inbound(k, a_send, a_recv, a_ssem, a_rsem).wait_recv()
        inbound(k, p_send, p_recv, p_ssem, p_rsem).wait_recv()
        live = (slot_of < a_recv[k]).astype(jnp.float32)
        p0, p1, p2 = p_recv[k, 0], p_recv[k, 1], p_recv[k, 2]
        resid = n0 * (p0 - q0) + n1 * (p1 - q1) + n2 * (p2 - q2)
        weight = live / (1.0 + resid * resid)
        jacob = [p1 * n2 - p2 * n1, p2 * n0 - p0 * n2, p0 * n1 - p1 * n0, n0, n1, n2]
        scaled = [weight * entry for entry in jacob]
        for e, (i, j) in enumerate(ENTRIES):
            prods[pl.ds(e * 8, 8), :] = scaled[i] * jacob[j]
        for i in range(6):
            prods[pl.ds((21 + i) * 8, 8), :] = scaled[i] * resid
        spread = jnp.zeros((8, LANES), jnp.float32)
        for g in range(4):
            some = prods[pl.ds(g * 64, 8, stride=8), :]
            for t in range(1, 8):
                some = some + prods[pl.ds(g * 64 + t, 8, stride=8), :]
            whole = jnp.sum(some, axis=1, keepdims=True)
            spread = spread + jnp.where(entry_of == sub + g * 8, whole, 0.0)
        line = jnp.sum(spread, axis=0, keepdims=True)
        r_send[k] = line
        for half in range(2):
            returned(k, half).start()
        return tsum + line

    tsum = lax.fori_loop(0, rounds, one_pair, jnp.zeros((1, LANES), jnp.float32))
    t_send[...] = tsum
    exchange = pltpu.make_async_remote_copy(
        src_ref=t_send, dst_ref=t_recv, send_sem=t_ssem, recv_sem=t_rsem,
        device_id=(me, 1 - rep), device_id_type=MESH,
    )
    exchange.start()

    source_sum = jnp.zeros((1, LANES), jnp.float32)
    for k in reversed(order):
        for half in range(2):
            pltpu.make_async_remote_copy(
                src_ref=r_send.at[k], dst_ref=r_recv.at[half, k],
                send_sem=r_ssem.at[half, k], recv_sem=r_rsem.at[half, k],
                device_id=(up(k + 1), half), device_id_type=MESH,
            ).wait_recv()
        both = r_recv[0, k] + r_recv[1, k]
        out_ref[pl.ds(k, 1), :] = both
        source_sum = source_sum + both
    exchange.wait_recv()
    target_sum = t_send[...] + t_recv[...]
    lane1 = lax.broadcasted_iota(jnp.int32, (1, LANES), 1)
    out_ref[pl.ds(rounds, 1), :] = source_sum + jnp.where(lane1 < 36, target_sum, -target_sum)

    for _, copy in sends:
        copy.wait_send()
    for k in order:
        for half in range(2):
            returned(k, half).wait_send()
    exchange.wait_send()


def finish(rounds, total_slots, sums_ref, diag_ref, grad_ref, pair_ref):
    pair_ref[...] = sums_ref[:rounds, :36] * (1.0 / total_slots)
    total = sums_ref[rounds : rounds + 1] * (1.0 / (total_slots * 2.0 * rounds))
    diag_ref[...] = total[:, :36]
    grad_ref[...] = total[:, 36:42]


def solution(mesh):
    n_blk = mesh.shape["blk"]

    def body(points, normals, src_block, tgt_index, active):
        npts = points.shape[2]
        rounds, nslots = src_block.shape[0], src_block.shape[3]
        rows = npts // LANES
        f32, i32 = jnp.float32, jnp.int32
        dma = pltpu.SemaphoreType.DMA
        total_slots = 2 * nslots * LANES
        sums = pl.pallas_call(
            functools.partial(kernel, n_blk, rounds, nslots, npts),
            out_shape=jax.ShapeDtypeStruct((rounds + 8, LANES), f32),
            in_specs=[pl.BlockSpec(memory_space=pl.ANY)] * 5,
            out_specs=pl.BlockSpec(memory_space=pltpu.VMEM),
            scratch_shapes=[
                pltpu.VMEM((3, rows, LANES), f32),
                pltpu.VMEM((3, rows, LANES), f32),
                pltpu.VMEM((rounds, nslots, LANES), i32),
                pltpu.SMEM((rounds, nslots), i32),
                pltpu.SMEM((1, rounds), i32),
                pltpu.VMEM((rounds, 3, nslots, LANES), f32),
                pltpu.VMEM((rounds, 1, LANES), i32),
                pltpu.VMEM((rounds, nslots, LANES), i32),
                pltpu.VMEM((rounds, 3, nslots, LANES), f32),
                pltpu.VMEM((rounds, 1, LANES), i32),
                pltpu.VMEM((256, LANES), f32),
                pltpu.VMEM((rounds, 1, LANES), f32),
                pltpu.VMEM((2, rounds, 1, LANES), f32),
                pltpu.VMEM((1, LANES), f32),
                pltpu.VMEM((1, LANES), f32),
                dma((5,)),
                dma((rounds,)), dma((rounds,)),
                dma((rounds,)), dma((rounds,)),
                dma((rounds,)), dma((rounds,)),
                dma((2, rounds)), dma((2, rounds)),
                dma, dma,
            ],
            compiler_params=pltpu.CompilerParams(collective_id=0, has_side_effects=True, vmem_limit_bytes=8 * 1024 * 1024),
        )(
            pltpu.with_memory_space_constraint(points.reshape(3, rows, LANES), pltpu.HBM),
            pltpu.with_memory_space_constraint(normals.reshape(3, rows, LANES), pltpu.HBM),
            pltpu.with_memory_space_constraint(src_block.reshape(rounds, nslots), pltpu.HBM),
            pltpu.with_memory_space_constraint(tgt_index.reshape(rounds, nslots, LANES), pltpu.HBM),
            pltpu.with_memory_space_constraint(active.reshape(1, rounds), pltpu.HBM),
        )
        diag, grad, pair = pl.pallas_call(
            functools.partial(finish, rounds, total_slots),
            out_shape=(
                jax.ShapeDtypeStruct((1, 36), f32),
                jax.ShapeDtypeStruct((1, 6), f32),
                jax.ShapeDtypeStruct((rounds, 36), f32),
            ),
            compiler_params=pltpu.CompilerParams(vmem_limit_bytes=1024 * 1024),
        )(sums)
        return diag, grad, pair.reshape(rounds, 1, 1, 36)

    return jax.shard_map(
        body,
        mesh=mesh,
        in_specs=(
            P("blk", None, None),
            P("blk", None, None),
            P(None, "blk", None, "rep"),
            P(None, "blk", None, "rep", None),
            P(None, "blk", None),
        ),
        out_specs=(P("blk", None), P("blk", None), P(None, "blk", None, None)),
        check_vma=False,
    )
```

```python
import functools

import jax
import jax.numpy as jnp
from jax import lax
from jax.experimental import pallas as pl
from jax.experimental.pallas import tpu as pltpu
from jax.sharding import PartitionSpec as P

MESH = pl.DeviceIdType.MESH
LANES = 128
ENTRIES = [(i, j) for i in range(6) for j in range(i, 6)]


def kernel(
    n_blk, rounds, nslots, npts,
    pts_hbm, nrm_hbm, src_hbm, tgt_hbm, act_hbm,
    out_ref,
    pts, nrm, tgt, src, act,
    p_send, a_send, i_recv, p_recv, a_recv,
    prods, r_send, r_recv, t_send, t_recv,
    local_sem, i_ssem, i_rsem, p_ssem, p_rsem, a_ssem, a_rsem,
    r_ssem, r_rsem, t_ssem, t_rsem,
):
    me = lax.axis_index("blk")
    rep = lax.axis_index("rep")
    rows = npts // LANES

    def up(k):
        return lax.rem(me + k, n_blk)

    def down(k):
        return lax.rem(me + n_blk - k, n_blk)

    barrier = pltpu.get_barrier_semaphore()
    for k in range(1, rounds + 1):
        pl.semaphore_signal(barrier, inc=1, device_id=(up(k), rep), device_id_type=MESH)
    pl.semaphore_signal(barrier, inc=1, device_id=(me, 1 - rep), device_id_type=MESH)

    loads = [
        pltpu.make_async_copy(src_hbm, src, local_sem.at[0]),
        pltpu.make_async_copy(act_hbm, act, local_sem.at[1]),
        pltpu.make_async_copy(pts_hbm, pts, local_sem.at[2]),
        pltpu.make_async_copy(tgt_hbm, tgt, local_sem.at[3]),
        pltpu.make_async_copy(nrm_hbm, nrm, local_sem.at[4]),
    ]
    for load in loads:
        load.start()
    for load in loads:
        load.wait()

    for k in range(rounds):
        for j in range(nslots):
            block = src[k, j]
            for c in range(3):
                p_send[k, c, pl.ds(j, 1), :] = pts[c, pl.ds(block, 1), :]
        a_send[k] = jnp.full((1, LANES), act[0, k], jnp.int32)

    pl.semaphore_wait(barrier, rounds + 1)

    sends = []
    order = list(range(rounds))
    for k in order:
        to = (down(k + 1), rep)
        for source, target, ssem, rsem in (
            (tgt.at[k], i_recv.at[k], i_ssem.at[k], i_rsem.at[k]),
            (a_send.at[k], a_recv.at[k], a_ssem.at[k], a_rsem.at[k]),
            (p_send.at[k], p_recv.at[k], p_ssem.at[k], p_rsem.at[k]),
        ):
            copy = pltpu.make_async_remote_copy(
                src_ref=source, dst_ref=target, send_sem=ssem, recv_sem=rsem,
                device_id=to, device_id_type=MESH,
            )
            copy.start()
            sends.append((k, copy))

    sub = lax.broadcasted_iota(jnp.int32, (nslots, LANES), 0)
    lane = lax.broadcasted_iota(jnp.int32, (nslots, LANES), 1)
    slot_of = sub + rep * nslots
    li, lj = lane // 6, lane % 6
    lo, hi = jnp.minimum(li, lj), jnp.maximum(li, lj)
    entry_of = jnp.where(
        lane < 36, lo * 6 - (lo * (lo - 1)) // 2 + hi - lo,
        jnp.where(lane < 42, lane - 36 + 21, -1),
    )

    def inbound(k, source, target, ssem, rsem):
        return pltpu.make_async_remote_copy(
            src_ref=source.at[k], dst_ref=target.at[k], send_sem=ssem.at[k], recv_sem=rsem.at[k],
            device_id=(down(k + 1), rep), device_id_type=MESH,
        )

    def returned(k, half):
        return pltpu.make_async_remote_copy(
            src_ref=r_send.at[k], dst_ref=r_recv.at[rep, k],
            send_sem=r_ssem.at[half, k], recv_sem=r_rsem.at[rep, k],
            device_id=(up(k + 1), half), device_id_type=MESH,
        )

    def one_pair(step, tsum):
        k = step
        inbound(k, tgt, i_recv, i_ssem, i_rsem).wait_recv()
        index = i_recv[k]
        row_of = lax.shift_right_logical(index, 7)
        lane_of = lax.bitwise_and(index, LANES - 1)
        acc = [jnp.zeros((nslots, LANES), jnp.float32)] * 6
        for row in range(rows):
            here = row_of == row
            for e, (table, c) in enumerate(((pts, 0), (pts, 1), (pts, 2), (nrm, 0), (nrm, 1), (nrm, 2))):
                line = jnp.broadcast_to(table[c, row : row + 1, :], (nslots, LANES))
                got = jnp.take_along_axis(line, lane_of, axis=1, mode="promise_in_bounds")
                acc[e] = jnp.where(here, got, acc[e])
        q0, q1, q2, n0, n1, n2 = acc

        inbound(k, a_send, a_recv, a_ssem, a_rsem).wait_recv()
        inbound(k, p_send, p_recv, p_ssem, p_rsem).wait_recv()
        live = (slot_of < a_recv[k]).astype(jnp.float32)
        p0, p1, p2 = p_recv[k, 0], p_recv[k, 1], p_recv[k, 2]
        resid = n0 * (p0 - q0) + n1 * (p1 - q1) + n2 * (p2 - q2)
        weight = live / (1.0 + resid * resid)
        jacob = [p1 * n2 - p2 * n1, p2 * n0 - p0 * n2, p0 * n1 - p1 * n0, n0, n1, n2]
        scaled = [weight * entry for entry in jacob]
        for e, (i, j) in enumerate(ENTRIES):
            prods[pl.ds(e * 8, 8), :] = scaled[i] * jacob[j]
        for i in range(6):
            prods[pl.ds((21 + i) * 8, 8), :] = scaled[i] * resid
        spread = jnp.zeros((8, LANES), jnp.float32)
        for g in range(4):
            some = prods[pl.ds(g * 64, 8, stride=8), :]
            for t in range(1, 8):
                some = some + prods[pl.ds(g * 64 + t, 8, stride=8), :]
            whole = jnp.sum(some, axis=1, keepdims=True)
            spread = spread + jnp.where(entry_of == sub + g * 8, whole, 0.0)
        line = jnp.sum(spread, axis=0, keepdims=True)
        r_send[k] = line
        for half in range(2):
            returned(k, half).start()
        return tsum + line

    tsum = lax.fori_loop(0, rounds, one_pair, jnp.zeros((1, LANES), jnp.float32))
    t_send[...] = tsum
    exchange = pltpu.make_async_remote_copy(
        src_ref=t_send, dst_ref=t_recv, send_sem=t_ssem, recv_sem=t_rsem,
        device_id=(me, 1 - rep), device_id_type=MESH,
    )
    exchange.start()

    source_sum = jnp.zeros((1, LANES), jnp.float32)
    for k in reversed(order):
        for half in range(2):
            pltpu.make_async_remote_copy(
                src_ref=r_send.at[k], dst_ref=r_recv.at[half, k],
                send_sem=r_ssem.at[half, k], recv_sem=r_rsem.at[half, k],
                device_id=(up(k + 1), half), device_id_type=MESH,
            ).wait_recv()
        both = r_recv[0, k] + r_recv[1, k]
        out_ref[pl.ds(k, 1), :] = both
        source_sum = source_sum + both
    exchange.wait_recv()
    target_sum = t_send[...] + t_recv[...]
    lane1 = lax.broadcasted_iota(jnp.int32, (1, LANES), 1)
    out_ref[pl.ds(rounds, 1), :] = source_sum + jnp.where(lane1 < 36, target_sum, -target_sum)

    for _, copy in sends:
        copy.wait_send()
    for k in order:
        for half in range(2):
            returned(k, half).wait_send()
    exchange.wait_send()


def finish(rounds, total_slots, sums_ref, diag_ref, grad_ref, pair_ref):
    pair_ref[...] = sums_ref[:rounds, :36] * (1.0 / total_slots)
    total = sums_ref[rounds : rounds + 1] * (1.0 / (total_slots * 2.0 * rounds))
    diag_ref[...] = total[:, :36]
    grad_ref[...] = total[:, 36:42]


def solution(mesh):
    n_blk = mesh.shape["blk"]

    def body(points, normals, src_block, tgt_index, active):
        npts = points.shape[2]
        rounds, nslots = src_block.shape[0], src_block.shape[3]
        rows = npts // LANES
        f32, i32 = jnp.float32, jnp.int32
        dma = pltpu.SemaphoreType.DMA
        total_slots = 2 * nslots * LANES
        sums = pl.pallas_call(
            functools.partial(kernel, n_blk, rounds, nslots, npts),
            out_shape=jax.ShapeDtypeStruct((rounds + 8, LANES), f32),
            in_specs=[pl.BlockSpec(memory_space=pl.ANY)] * 5,
            out_specs=pl.BlockSpec(memory_space=pltpu.VMEM),
            scratch_shapes=[
                pltpu.VMEM((3, rows, LANES), f32),
                pltpu.VMEM((3, rows, LANES), f32),
                pltpu.VMEM((rounds, nslots, LANES), i32),
                pltpu.SMEM((rounds, nslots), i32),
                pltpu.SMEM((1, rounds), i32),
                pltpu.VMEM((rounds, 3, nslots, LANES), f32),
                pltpu.VMEM((rounds, 1, LANES), i32),
                pltpu.VMEM((rounds, nslots, LANES), i32),
                pltpu.VMEM((rounds, 3, nslots, LANES), f32),
                pltpu.VMEM((rounds, 1, LANES), i32),
                pltpu.VMEM((256, LANES), f32),
                pltpu.VMEM((rounds, 1, LANES), f32),
                pltpu.VMEM((2, rounds, 1, LANES), f32),
                pltpu.VMEM((1, LANES), f32),
                pltpu.VMEM((1, LANES), f32),
                dma((5,)),
                dma((rounds,)), dma((rounds,)),
                dma((rounds,)), dma((rounds,)),
                dma((rounds,)), dma((rounds,)),
                dma((2, rounds)), dma((2, rounds)),
                dma, dma,
            ],
            compiler_params=pltpu.CompilerParams(collective_id=0, has_side_effects=True, vmem_limit_bytes=8 * 1024 * 1024),
        )(
            pltpu.with_memory_space_constraint(points.reshape(3, rows, LANES), pltpu.HBM),
            pltpu.with_memory_space_constraint(normals.reshape(3, rows, LANES), pltpu.HBM),
            pltpu.with_memory_space_constraint(src_block.reshape(rounds, nslots), pltpu.HBM),
            pltpu.with_memory_space_constraint(tgt_index.reshape(rounds, nslots, LANES), pltpu.HBM),
            pltpu.with_memory_space_constraint(active.reshape(1, rounds), pltpu.HBM),
        )
        diag, grad, pair = pl.pallas_call(
            functools.partial(finish, rounds, total_slots),
            out_shape=(
                jax.ShapeDtypeStruct((1, 36), f32),
                jax.ShapeDtypeStruct((1, 6), f32),
                jax.ShapeDtypeStruct((rounds, 36), f32),
            ),
            compiler_params=pltpu.CompilerParams(vmem_limit_bytes=1024 * 1024),
        )(sums)
        return diag, grad, pair.reshape(rounds, 1, 1, 36)

    return jax.shard_map(
        body,
        mesh=mesh,
        in_specs=(
            P("blk", None, None),
            P("blk", None, None),
            P(None, "blk", None, "rep"),
            P(None, "blk", None, "rep", None),
            P(None, "blk", None),
        ),
        out_specs=(P("blk", None), P("blk", None), P(None, "blk", None, None)),
        check_vma=False,
    )
```

```python
import functools

import jax
import jax.numpy as jnp
from jax import lax
from jax.experimental import pallas as pl
from jax.experimental.pallas import tpu as pltpu
from jax.sharding import PartitionSpec as P

MESH = pl.DeviceIdType.MESH
LANES = 128
SIDE = 4
ENTRIES = [(i, j) for i in range(6) for j in range(i, 6)]


def kernel(
    n_blk, rounds, nslots, npts, side,
    pts_hbm, nrm_hbm, src_hbm, tgt_hbm, act_hbm,
    out_ref,
    tab, tgt, src, act,
    p_send, a_send, i_recv, p_recv, a_recv,
    prods, r_send, r_recv, t_send, t_recv,
    local_sem, i_ssem, i_rsem, p_ssem, p_rsem, a_ssem, a_rsem,
    r_ssem, r_rsem, t_ssem, t_rsem, f_ssem, late_sem,
):
    me = lax.axis_index("blk")
    rep = lax.axis_index("rep")
    rows = npts // LANES
    order = range(rounds)
    is_late = me >= n_blk - rounds
    is_helper = me < rounds
    is_own = me < side
    late_of_me = me + n_blk - jnp.where(is_own, side, rounds + side)
    plane = side * side
    is_post = jnp.logical_and(me >= plane - rounds, me < plane)
    helper_of_post = me - jnp.where(me < plane - side, side, rounds + side)

    def near(k):
        return me + k < n_blk

    def helps(k):
        return jnp.logical_and(is_helper, late_of_me + k >= n_blk)

    def helped(k):
        return late_of_me + k - n_blk

    def host(k):
        return me - k + jnp.where(me >= k, 0, jnp.where(me >= k - side, side, rounds + side))

    def copy_to(source, target, ssem, rsem, blk, core):
        return pltpu.make_async_remote_copy(
            src_ref=source, dst_ref=target, send_sem=ssem, recv_sem=rsem,
            device_id=(blk, core), device_id_type=MESH,
        )

    loads = [
        pltpu.make_async_copy(src_hbm, src, local_sem.at[0]),
        pltpu.make_async_copy(act_hbm, act, local_sem.at[1]),
        pltpu.make_async_copy(pts_hbm, tab.at[0], local_sem.at[2]),
        pltpu.make_async_copy(tgt_hbm, tgt, local_sem.at[3]),
        pltpu.make_async_copy(nrm_hbm, tab.at[1], local_sem.at[4]),
    ]

    barrier = pltpu.get_barrier_semaphore()

    def greet(blk, core):
        pl.semaphore_signal(barrier, inc=1, device_id=(blk, core), device_id_type=MESH)

    for load in loads:
        load.start()

    @pl.when(is_late)
    def _():
        greet(me - n_blk + plane, rep)

    @pl.when(is_helper)
    def _():
        greet(late_of_me - n_blk + plane, rep)

    greet(me, 1 - rep)
    for k in range(1, rounds + 1):
        @pl.when(near(k))
        def _():
            greet(me + k, rep)

        if k != side:
            @pl.when(helps(k))
            def _():
                greet(helped(k), rep)

    @pl.when(is_post)
    def _():
        pl.semaphore_wait(barrier, rounds + 3)
        pl.semaphore_signal(late_sem, inc=1, device_id=(helper_of_post, rep), device_id_type=MESH)

    for load in loads:
        load.wait()

    for k in order:
        for j in range(nslots):
            block = src[k, j]
            for c in range(3):
                p_send[k, c, pl.ds(j, 1), :] = tab[0, c, pl.ds(block, 1), :]
        a_send[k] = jnp.full((1, LANES), act[0, k], jnp.int32)

    @pl.when(jnp.logical_not(is_post))
    def _():
        pl.semaphore_wait(barrier, rounds + jnp.where(is_own, 0, 1))

    def outbound(k):
        blk = host(k + 1)
        slot = k + jnp.where(me < k + 1, rounds, 0)
        return [
            copy_to(tgt.at[k], i_recv.at[slot], i_ssem.at[k], i_rsem.at[slot], blk, rep),
            copy_to(a_send.at[k], a_recv.at[slot], a_ssem.at[k], a_rsem.at[slot], blk, rep),
            copy_to(p_send.at[k], p_recv.at[slot], p_ssem.at[k], p_rsem.at[slot], blk, rep),
        ]

    def arrival(source, target, ssem, rsem, k, slot):
        copy_to(source.at[k], target.at[slot], ssem.at[k], rsem.at[slot], host(k + 1), rep).wait_recv()

    for k in order:
        @pl.when(jnp.logical_not(jnp.logical_and(is_own, k + 1 == side)))
        def _():
            for copy in outbound(k):
                copy.start()

    sub = lax.broadcasted_iota(jnp.int32, (nslots, LANES), 0)
    lane = lax.broadcasted_iota(jnp.int32, (nslots, LANES), 1)
    slot_of = sub + rep * nslots
    li, lj = lane // 6, lane % 6
    lo, hi = jnp.minimum(li, lj), jnp.maximum(li, lj)
    entry_of = jnp.where(
        lane < 36, lo * 6 - (lo * (lo - 1)) // 2 + hi - lo,
        jnp.where(lane < 42, lane - 36 + 21, -1),
    )

    def forwards(k):
        slot = k + rounds
        parts = ((tgt, i_recv, i_rsem), (a_send, a_recv, a_rsem), (p_send, p_recv, p_rsem))
        return [
            copy_to(
                mine.at[k] if k + 1 == side else ref.at[slot],
                ref.at[k], f_ssem.at[e, k], rsem.at[k], late_of_me, rep,
            )
            for e, (mine, ref, rsem) in enumerate(parts)
        ]

    @pl.when(is_helper)
    def _():
        pl.semaphore_wait(late_sem, 1)
        for step in order:
            for k in order:
                @pl.when(jnp.logical_and(helps(k + 1), helped(k + 1) == step // 2 + step % 2 * side))
                def _():
                    if k + 1 != side:
                        arrival(tgt, i_recv, i_ssem, i_rsem, k, k + rounds)
                        arrival(a_send, a_recv, a_ssem, a_rsem, k, k + rounds)
                        arrival(p_send, p_recv, p_ssem, p_rsem, k, k + rounds)
                    for copy in forwards(k):
                        copy.start()

    def returned(k, half):
        return copy_to(
            r_send.at[k], r_recv.at[rep, k], r_ssem.at[half, k], r_rsem.at[rep, k],
            lax.rem(me + k + 1, n_blk), half,
        )

    def turn(step):
        source = jnp.where(me >= n_blk - 2, (step % 2) * side + step // 2, step)
        return jnp.where(is_late, lax.rem(source + n_blk - 1 - me, rounds), step)

    def gather(k):
        arrival(tgt, i_recv, i_ssem, i_rsem, k, k)
        index = i_recv[k]
        row_of = lax.shift_right_logical(index, 7)
        lane_of = lax.bitwise_and(index, LANES - 1)
        acc = [jnp.zeros((nslots, LANES), jnp.float32)] * 6
        for row in range(rows):
            here = row_of == row
            for e in range(6):
                line = jnp.broadcast_to(tab[e // 3, e % 3, row : row + 1, :], (nslots, LANES))
                got = jnp.take_along_axis(line, lane_of, axis=1, mode="promise_in_bounds")
                acc[e] = jnp.where(here, got, acc[e])
        return tuple(acc)

    def await_points(k):
        arrival(a_send, a_recv, a_ssem, a_rsem, k, k)
        arrival(p_send, p_recv, p_ssem, p_rsem, k, k)

    def gram(k, picked):
        q0, q1, q2, n0, n1, n2 = picked
        live = (slot_of < a_recv[k]).astype(jnp.float32)
        p0, p1, p2 = p_recv[k, 0], p_recv[k, 1], p_recv[k, 2]
        resid = n0 * (p0 - q0) + n1 * (p1 - q1) + n2 * (p2 - q2)
        weight = live / (1.0 + resid * resid)
        jacob = [p1 * n2 - p2 * n1, p2 * n0 - p0 * n2, p0 * n1 - p1 * n0, n0, n1, n2]
        scaled = [weight * entry for entry in jacob]
        for e, (i, j) in enumerate(ENTRIES):
            prods[pl.ds(e * 8, 8), :] = scaled[i] * jacob[j]
        for i in range(6):
            prods[pl.ds((21 + i) * 8, 8), :] = scaled[i] * resid
        spread = jnp.zeros((8, LANES), jnp.float32)
        for g in range(4):
            some = prods[pl.ds(g * 64, 8, stride=8), :]
            for t in range(1, 8):
                some = some + prods[pl.ds(g * 64 + t, 8, stride=8), :]
            whole = jnp.sum(some, axis=1, keepdims=True)
            spread = spread + jnp.where(entry_of == sub + g * 8, whole, 0.0)
        line = jnp.sum(spread, axis=0, keepdims=True)
        r_send[k] = line
        return line

    def give_back(k):
        for half in range(2):
            returned(k, half).start()

    def one_step(step, carry):
        picked, tsum = carry[:6], carry[6]
        before, k = turn(step - 1), turn(step)
        await_points(before)
        arrived = gather(k)
        line = gram(before, picked)
        give_back(before)
        return arrived + (tsum + line,)

    first = gather(turn(0))
    carry = lax.fori_loop(1, rounds, one_step, first + (jnp.zeros((1, LANES), jnp.float32),))
    last = turn(rounds - 1)
    await_points(last)
    line = gram(last, carry[:6])
    give_back(last)
    t_send[...] = carry[6] + line

    exchange = copy_to(t_send, t_recv, t_ssem, t_rsem, me, 1 - rep)
    exchange.start()

    source_sum = jnp.zeros((1, LANES), jnp.float32)
    for k in order:
        for half in range(2):
            copy_to(
                r_send.at[k], r_recv.at[half, k], r_ssem.at[half, k], r_rsem.at[half, k], host(k + 1), half
            ).wait_recv()
        both = r_recv[0, k] + r_recv[1, k]
        out_ref[pl.ds(k, 1), :] = both
        source_sum = source_sum + both
    exchange.wait_recv()
    target_sum = t_send[...] + t_recv[...]
    lane1 = lax.broadcasted_iota(jnp.int32, (1, LANES), 1)
    out_ref[pl.ds(rounds, 1), :] = source_sum + jnp.where(lane1 < 36, target_sum, -target_sum)

    for k in order:
        @pl.when(jnp.logical_not(jnp.logical_and(is_own, k + 1 == side)))
        def _():
            for copy in outbound(k):
                copy.wait_send()

    for k in order:
        for half in range(2):
            returned(k, half).wait_send()
    exchange.wait_send()

    @pl.when(is_helper)
    def _():
        for k in order:
            @pl.when(helps(k + 1))
            def _():
                for copy in forwards(k):
                    copy.wait_send()


def finish(rounds, total_slots, sums_ref, diag_ref, grad_ref, pair_ref):
    pair_ref[...] = sums_ref[:rounds, :36] * (1.0 / total_slots)
    total = sums_ref[rounds : rounds + 1] * (1.0 / (total_slots * 2.0 * rounds))
    diag_ref[...] = total[:, :36]
    grad_ref[...] = total[:, 36:42]


def solution(mesh):
    n_blk = mesh.shape["blk"]

    def body(points, normals, src_block, tgt_index, active):
        npts = points.shape[2]
        rounds, nslots = src_block.shape[0], src_block.shape[3]
        rows = npts // LANES
        f32, i32 = jnp.float32, jnp.int32
        dma = pltpu.SemaphoreType.DMA
        total_slots = 2 * nslots * LANES
        sums = pl.pallas_call(
            functools.partial(kernel, n_blk, rounds, nslots, npts, SIDE),
            out_shape=jax.ShapeDtypeStruct((rounds + 8, LANES), f32),
            in_specs=[pl.BlockSpec(memory_space=pl.ANY)] * 5,
            out_specs=pl.BlockSpec(memory_space=pltpu.VMEM),
            scratch_shapes=[
                pltpu.VMEM((2, 3, rows, LANES), f32),
                pltpu.VMEM((rounds, nslots, LANES), i32),
                pltpu.SMEM((rounds, nslots), i32),
                pltpu.SMEM((1, rounds), i32),
                pltpu.VMEM((rounds, 3, nslots, LANES), f32),
                pltpu.VMEM((rounds, 1, LANES), i32),
                pltpu.VMEM((2 * rounds, nslots, LANES), i32),
                pltpu.VMEM((2 * rounds, 3, nslots, LANES), f32),
                pltpu.VMEM((2 * rounds, 1, LANES), i32),
                pltpu.VMEM((256, LANES), f32),
                pltpu.VMEM((rounds, 1, LANES), f32),
                pltpu.VMEM((2, rounds, 1, LANES), f32),
                pltpu.VMEM((1, LANES), f32),
                pltpu.VMEM((1, LANES), f32),
                dma((5,)),
                dma((rounds,)), dma((2 * rounds,)),
                dma((rounds,)), dma((2 * rounds,)),
                dma((rounds,)), dma((2 * rounds,)),
                dma((2, rounds)), dma((2, rounds)),
                dma, dma, dma((3, rounds)), pltpu.SemaphoreType.REGULAR,
            ],
            compiler_params=pltpu.CompilerParams(collective_id=0, has_side_effects=True, vmem_limit_bytes=8 * 1024 * 1024),
        )(
            pltpu.with_memory_space_constraint(points.reshape(3, rows, LANES), pltpu.HBM),
            pltpu.with_memory_space_constraint(normals.reshape(3, rows, LANES), pltpu.HBM),
            pltpu.with_memory_space_constraint(src_block.reshape(rounds, nslots), pltpu.HBM),
            pltpu.with_memory_space_constraint(tgt_index.reshape(rounds, nslots, LANES), pltpu.HBM),
            pltpu.with_memory_space_constraint(active.reshape(1, rounds), pltpu.HBM),
        )
        diag, grad, pair = pl.pallas_call(
            functools.partial(finish, rounds, total_slots),
            out_shape=(
                jax.ShapeDtypeStruct((1, 36), f32),
                jax.ShapeDtypeStruct((1, 6), f32),
                jax.ShapeDtypeStruct((rounds, 36), f32),
            ),
            compiler_params=pltpu.CompilerParams(vmem_limit_bytes=1024 * 1024),
        )(sums)
        return diag, grad, pair.reshape(rounds, 1, 1, 36)

    return jax.shard_map(
        body,
        mesh=mesh,
        in_specs=(
            P("blk", None, None),
            P("blk", None, None),
            P(None, "blk", None, "rep"),
            P(None, "blk", None, "rep", None),
            P(None, "blk", None),
        ),
        out_specs=(P("blk", None), P("blk", None), P(None, "blk", None, None)),
        check_vma=False,
    )
```

```python
import functools

import jax
import jax.numpy as jnp
from jax import lax
from jax.experimental import pallas as pl
from jax.experimental.pallas import tpu as pltpu
from jax.sharding import PartitionSpec as P

MESH = pl.DeviceIdType.MESH
LANES = 128
SIDE = 4
ENTRIES = [(i, j) for i in range(6) for j in range(i, 6)]


def kernel(
    n_blk, rounds, nslots, npts, side,
    pts_hbm, nrm_hbm, src_hbm, tgt_hbm, act_hbm,
    out_ref,
    tab, tgt, src, act,
    m_send, m_recv,
    prods, r_send, r_recv, t_send, t_recv,
    local_sem, m_ssem, m_rsem,
    r_ssem, r_rsem, t_ssem, t_rsem, f_ssem, late_sem,
):
    me = lax.axis_index("blk")
    rep = lax.axis_index("rep")
    rows = npts // LANES
    order = range(rounds)
    far_first = (6, 7, 5, 2, 8, 3, 1, 4)
    is_late = me >= n_blk - rounds
    is_helper = me < rounds
    is_own = me < side
    late_of_me = me + n_blk - jnp.where(is_own, side, rounds + side)
    plane = side * side
    is_post = jnp.logical_and(me >= plane - rounds, me < plane)
    helper_of_post = me - jnp.where(me < plane - side, side, rounds + side)

    def near(k):
        return me + k < n_blk

    def helps(k):
        return jnp.logical_and(is_helper, late_of_me + k >= n_blk)

    def helped(k):
        return late_of_me + k - n_blk

    def host(k):
        return me - k + jnp.where(me >= k, 0, jnp.where(me >= k - side, side, rounds + side))

    def copy_to(source, target, ssem, rsem, blk, core):
        return pltpu.make_async_remote_copy(
            src_ref=source, dst_ref=target, send_sem=ssem, recv_sem=rsem,
            device_id=(blk, core), device_id_type=MESH,
        )

    loads = [
        pltpu.make_async_copy(src_hbm, src, local_sem.at[0]),
        pltpu.make_async_copy(act_hbm, act, local_sem.at[1]),
        pltpu.make_async_copy(pts_hbm, tab.at[0], local_sem.at[2]),
        pltpu.make_async_copy(tgt_hbm, tgt, local_sem.at[3]),
        pltpu.make_async_copy(nrm_hbm, tab.at[1], local_sem.at[4]),
    ]

    barrier = pltpu.get_barrier_semaphore()

    def greet(blk, core):
        pl.semaphore_signal(barrier, inc=1, device_id=(blk, core), device_id_type=MESH)

    @pl.when(is_late)
    def _():
        greet(me - n_blk + plane, rep)

    for load in loads:
        load.start()

    @pl.when(is_helper)
    def _():
        greet(late_of_me - n_blk + plane, rep)

    greet(me, 1 - rep)
    for k in far_first:
        @pl.when(near(k))
        def _():
            greet(me + k, rep)

        if k != side:
            @pl.when(helps(k))
            def _():
                greet(helped(k), rep)

    @pl.when(is_post)
    def _():
        pl.semaphore_wait(barrier, rounds + 3)
        pl.semaphore_signal(late_sem, inc=1, device_id=(helper_of_post, rep), device_id_type=MESH)

    for load in loads:
        load.wait()

    for k in order:
        for j in range(nslots):
            block = src[k, j]
            for c in range(3):
                m_send[k, c, pl.ds(j, 1), :] = tab[0, c, pl.ds(block, 1), :]
        m_send[k, 3] = tgt[k].astype(jnp.float32)
        m_send[k, 4] = jnp.full((nslots, LANES), act[0, k].astype(jnp.float32), jnp.float32)

    @pl.when(jnp.logical_not(is_post))
    def _():
        pl.semaphore_wait(barrier, rounds + jnp.where(is_own, 0, 1))

    def outbound(k):
        slot = k + jnp.where(me < k + 1, rounds, 0)
        return copy_to(m_send.at[k], m_recv.at[slot], m_ssem.at[k], m_rsem.at[slot], host(k + 1), rep)

    def arrival(k, slot):
        copy_to(m_send.at[k], m_recv.at[slot], m_ssem.at[k], m_rsem.at[slot], host(k + 1), rep).wait_recv()

    for k in (far - 1 for far in far_first):
        @pl.when(jnp.logical_not(jnp.logical_and(is_own, k + 1 == side)))
        def _():
            outbound(k).start()

    sub = lax.broadcasted_iota(jnp.int32, (nslots, LANES), 0)
    lane = lax.broadcasted_iota(jnp.int32, (nslots, LANES), 1)
    slot_of = sub + rep * nslots
    li, lj = lane // 6, lane % 6
    lo, hi = jnp.minimum(li, lj), jnp.maximum(li, lj)
    entry_of = jnp.where(
        lane < 36, lo * 6 - (lo * (lo - 1)) // 2 + hi - lo,
        jnp.where(lane < 42, lane - 36 + 21, -1),
    )

    def forward(k):
        source = m_send.at[k] if k + 1 == side else m_recv.at[k + rounds]
        return copy_to(source, m_recv.at[k], f_ssem.at[k], m_rsem.at[k], late_of_me, rep)

    @pl.when(is_helper)
    def _():
        pl.semaphore_wait(late_sem, 1)
        for step in order:
            for k in order:
                @pl.when(jnp.logical_and(helps(k + 1), helped(k + 1) == step // 2 + step % 2 * side))
                def _():
                    if k + 1 != side:
                        arrival(k, k + rounds)
                    forward(k).start()

    def returned(k, half):
        return copy_to(
            r_send.at[k], r_recv.at[rep, k], r_ssem.at[half, k], r_rsem.at[rep, k],
            lax.rem(me + k + 1, n_blk), half,
        )

    def turn(step):
        source = jnp.where(me >= n_blk - 2, (step % 2) * side + step // 2, step)
        usual = step * 0
        for place, far in enumerate(far_first):
            usual = jnp.where(step == place, far - 1, usual)
        return jnp.where(is_late, lax.rem(source + n_blk - 1 - me, rounds), usual)

    def gather(k):
        arrival(k, k)
        index = m_recv[k, 3].astype(jnp.int32)
        row_of = lax.shift_right_logical(index, 7)
        lane_of = lax.bitwise_and(index, LANES - 1)
        acc = [jnp.zeros((nslots, LANES), jnp.float32)] * 6
        for row in range(rows):
            here = row_of == row
            for e in range(6):
                line = jnp.broadcast_to(tab[e // 3, e % 3, row : row + 1, :], (nslots, LANES))
                got = jnp.take_along_axis(line, lane_of, axis=1, mode="promise_in_bounds")
                acc[e] = jnp.where(here, got, acc[e])
        return tuple(acc)

    def gram(k, picked):
        q0, q1, q2, n0, n1, n2 = picked
        live = (slot_of < m_recv[k, 4].astype(jnp.int32)).astype(jnp.float32)
        p0, p1, p2 = m_recv[k, 0], m_recv[k, 1], m_recv[k, 2]
        resid = n0 * (p0 - q0) + n1 * (p1 - q1) + n2 * (p2 - q2)
        weight = live / (1.0 + resid * resid)
        jacob = [p1 * n2 - p2 * n1, p2 * n0 - p0 * n2, p0 * n1 - p1 * n0, n0, n1, n2]
        scaled = [weight * entry for entry in jacob]
        for e, (i, j) in enumerate(ENTRIES):
            prods[pl.ds(e * 8, 8), :] = scaled[i] * jacob[j]
        for i in range(6):
            prods[pl.ds((21 + i) * 8, 8), :] = scaled[i] * resid
        parts = []
        for g in range(4):
            some = prods[pl.ds(g * 64, 8, stride=8), :]
            for t in range(1, 8):
                some = some + prods[pl.ds(g * 64 + t, 8, stride=8), :]
            parts.append(some)
        whole = jnp.dot(
            jnp.concatenate(parts, axis=0), jnp.ones((LANES, LANES), jnp.float32),
            precision=lax.Precision.HIGHEST, preferred_element_type=jnp.float32,
        )
        spread = jnp.zeros((8, LANES), jnp.float32)
        for g in range(4):
            spread = spread + jnp.where(entry_of == sub + g * 8, whole[g * 8 : g * 8 + 8], 0.0)
        line = jnp.sum(spread, axis=0, keepdims=True)
        r_send[k] = line
        return line

    def give_back(k):
        for half in range(2):
            returned(k, half).start()

    def one_step(step, carry):
        picked, tsum = carry[:6], carry[6]
        before, k = turn(step - 1), turn(step)
        arrived = gather(k)
        line = gram(before, picked)
        give_back(before)
        return arrived + (tsum + line,)

    first = gather(turn(0))
    carry = lax.fori_loop(1, rounds, one_step, first + (jnp.zeros((1, LANES), jnp.float32),))
    last = turn(rounds - 1)
    line = gram(last, carry[:6])
    give_back(last)
    t_send[...] = carry[6] + line

    exchange = copy_to(t_send, t_recv, t_ssem, t_rsem, me, 1 - rep)
    exchange.start()

    source_sum = jnp.zeros((1, LANES), jnp.float32)
    for k in order:
        for half in range(2):
            copy_to(
                r_send.at[k], r_recv.at[half, k], r_ssem.at[half, k], r_rsem.at[half, k], host(k + 1), half
            ).wait_recv()
        both = r_recv[0, k] + r_recv[1, k]
        out_ref[pl.ds(k, 1), :] = both
        source_sum = source_sum + both
    exchange.wait_recv()
    target_sum = t_send[...] + t_recv[...]
    lane1 = lax.broadcasted_iota(jnp.int32, (1, LANES), 1)
    out_ref[pl.ds(rounds, 1), :] = source_sum + jnp.where(lane1 < 36, target_sum, -target_sum)

    for k in order:
        @pl.when(jnp.logical_not(jnp.logical_and(is_own, k + 1 == side)))
        def _():
            outbound(k).wait_send()

    for k in order:
        for half in range(2):
            returned(k, half).wait_send()
    exchange.wait_send()

    @pl.when(is_helper)
    def _():
        for k in order:
            @pl.when(helps(k + 1))
            def _():
                forward(k).wait_send()


def finish(rounds, total_slots, sums_ref, diag_ref, grad_ref, pair_ref):
    pair_ref[...] = sums_ref[:rounds, :36] * (1.0 / total_slots)
    total = sums_ref[rounds : rounds + 1] * (1.0 / (total_slots * 2.0 * rounds))
    diag_ref[...] = total[:, :36]
    grad_ref[...] = total[:, 36:42]


def solution(mesh):
    n_blk = mesh.shape["blk"]

    def body(points, normals, src_block, tgt_index, active):
        npts = points.shape[2]
        rounds, nslots = src_block.shape[0], src_block.shape[3]
        rows = npts // LANES
        f32, i32 = jnp.float32, jnp.int32
        dma = pltpu.SemaphoreType.DMA
        total_slots = 2 * nslots * LANES
        sums = pl.pallas_call(
            functools.partial(kernel, n_blk, rounds, nslots, npts, SIDE),
            out_shape=jax.ShapeDtypeStruct((rounds + 8, LANES), f32),
            in_specs=[pl.BlockSpec(memory_space=pl.ANY)] * 5,
            out_specs=pl.BlockSpec(memory_space=pltpu.VMEM),
            scratch_shapes=[
                pltpu.VMEM((2, 3, rows, LANES), f32),
                pltpu.VMEM((rounds, nslots, LANES), i32),
                pltpu.SMEM((rounds, nslots), i32),
                pltpu.SMEM((1, rounds), i32),
                pltpu.VMEM((rounds, 5, nslots, LANES), f32),
                pltpu.VMEM((2 * rounds, 5, nslots, LANES), f32),
                pltpu.VMEM((256, LANES), f32),
                pltpu.VMEM((rounds, 1, LANES), f32),
                pltpu.VMEM((2, rounds, 1, LANES), f32),
                pltpu.VMEM((1, LANES), f32),
                pltpu.VMEM((1, LANES), f32),
                dma((5,)),
                dma((rounds,)), dma((2 * rounds,)),
                dma((2, rounds)), dma((2, rounds)),
                dma, dma, dma((rounds,)), pltpu.SemaphoreType.REGULAR,
            ],
            compiler_params=pltpu.CompilerParams(collective_id=0, has_side_effects=True, vmem_limit_bytes=8 * 1024 * 1024),
        )(
            pltpu.with_memory_space_constraint(points.reshape(3, rows, LANES), pltpu.HBM),
            pltpu.with_memory_space_constraint(normals.reshape(3, rows, LANES), pltpu.HBM),
            pltpu.with_memory_space_constraint(src_block.reshape(rounds, nslots), pltpu.HBM),
            pltpu.with_memory_space_constraint(tgt_index.reshape(rounds, nslots, LANES), pltpu.HBM),
            pltpu.with_memory_space_constraint(active.reshape(1, rounds), pltpu.HBM),
        )
        diag, grad, pair = pl.pallas_call(
            functools.partial(finish, rounds, total_slots),
            out_shape=(
                jax.ShapeDtypeStruct((1, 36), f32),
                jax.ShapeDtypeStruct((1, 6), f32),
                jax.ShapeDtypeStruct((rounds, 36), f32),
            ),
            compiler_params=pltpu.CompilerParams(vmem_limit_bytes=1024 * 1024),
        )(sums)
        return diag, grad, pair.reshape(rounds, 1, 1, 36)

    return jax.shard_map(
        body,
        mesh=mesh,
        in_specs=(
            P("blk", None, None),
            P("blk", None, None),
            P(None, "blk", None, "rep"),
            P(None, "blk", None, "rep", None),
            P(None, "blk", None),
        ),
        out_specs=(P("blk", None), P("blk", None), P(None, "blk", None, None)),
        check_vma=False,
    )
```

```python
import functools

import jax
import jax.numpy as jnp
from jax import lax
from jax.experimental import pallas as pl
from jax.experimental.pallas import tpu as pltpu
from jax.sharding import PartitionSpec as P

MESH = pl.DeviceIdType.MESH
LANES = 128
SIDE = 4
ENTRIES = [(i, j) for i in range(6) for j in range(i, 6)]


def kernel(
    n_blk, rounds, nslots, npts, side,
    pts_hbm, nrm_hbm, src_hbm, tgt_hbm, act_hbm,
    out_ref,
    tab, tgt, src, act,
    m_send, m_recv, split, stage,
    prods, r_send, r_recv, t_send, t_recv,
    local_sem, m_ssem, m_rsem,
    r_ssem, r_rsem, t_ssem, t_rsem, f_ssem, late_sem,
):
    me = lax.axis_index("blk")
    rep = lax.axis_index("rep")
    rows = npts // LANES
    order = range(rounds)
    far_first = (6, 7, 5, 2, 8, 3, 1, 4)
    is_late = me >= n_blk - rounds
    is_helper = me < rounds
    is_own = me < side
    late_of_me = me + n_blk - jnp.where(is_own, side, rounds + side)
    plane = side * side
    is_post = jnp.logical_and(me >= plane - rounds, me < plane)
    helper_of_post = me - jnp.where(me < plane - side, side, rounds + side)

    def near(k):
        return me + k < n_blk

    def helps(k):
        return jnp.logical_and(is_helper, late_of_me + k >= n_blk)

    def helped(k):
        return late_of_me + k - n_blk

    def host(k):
        return me - k + jnp.where(me >= k, 0, jnp.where(me >= k - side, side, rounds + side))

    def copy_to(source, target, ssem, rsem, blk, core):
        return pltpu.make_async_remote_copy(
            src_ref=source, dst_ref=target, send_sem=ssem, recv_sem=rsem,
            device_id=(blk, core), device_id_type=MESH,
        )

    loads = [
        pltpu.make_async_copy(src_hbm, src, local_sem.at[0]),
        pltpu.make_async_copy(act_hbm, act, local_sem.at[1]),
        pltpu.make_async_copy(pts_hbm, tab.at[0], local_sem.at[2]),
        pltpu.make_async_copy(tgt_hbm, tgt, local_sem.at[3]),
        pltpu.make_async_copy(nrm_hbm, tab.at[1], local_sem.at[4]),
    ]

    barrier = pltpu.get_barrier_semaphore()

    def greet(blk, core):
        pl.semaphore_signal(barrier, inc=1, device_id=(blk, core), device_id_type=MESH)

    @pl.when(is_late)
    def _():
        greet(me - n_blk + plane, rep)

    for load in loads:
        load.start()

    @pl.when(is_helper)
    def _():
        greet(late_of_me - n_blk + plane, rep)

    greet(me, 1 - rep)
    for k in far_first:
        @pl.when(near(k))
        def _():
            greet(me + k, rep)

        if k != side:
            @pl.when(helps(k))
            def _():
                greet(helped(k), rep)

    @pl.when(is_post)
    def _():
        pl.semaphore_wait(barrier, rounds + 3)
        pl.semaphore_signal(late_sem, inc=1, device_id=(helper_of_post, rep), device_id_type=MESH)

    for load in loads:
        load.wait()

    for k in order:
        for j in range(nslots):
            block = src[k, j]
            for c in range(3):
                m_send[k, c, pl.ds(j, 1), :] = tab[0, c, pl.ds(block, 1), :]
        m_send[k, 3] = tgt[k].astype(jnp.float32)
        m_send[k, 4] = jnp.full((nslots, LANES), act[0, k].astype(jnp.float32), jnp.float32)

    @pl.when(jnp.logical_not(is_post))
    def _():
        pl.semaphore_wait(barrier, rounds + jnp.where(is_own, 0, 1))

    def outbound(k):
        slot = k + jnp.where(me < k + 1, rounds, 0)
        return copy_to(m_send.at[k], m_recv.at[slot], m_ssem.at[k], m_rsem.at[slot], host(k + 1), rep)

    def arrival(k, slot):
        copy_to(m_send.at[k], m_recv.at[slot], m_ssem.at[k], m_rsem.at[slot], host(k + 1), rep).wait_recv()

    for k in (far - 1 for far in far_first):
        @pl.when(jnp.logical_not(jnp.logical_and(is_own, k + 1 == side)))
        def _():
            outbound(k).start()

    for c in range(3):
        normal = jnp.concatenate(
            [tab[1, c, pl.ds(odd, rows // 2, stride=2), :] for odd in range(2)], axis=1
        )
        top = normal.astype(jnp.bfloat16)
        split[pl.ds(c * rows, rows // 2), :] = top
        split[pl.ds(c * rows + rows // 2, rows // 2), :] = (normal - top.astype(jnp.float32)).astype(jnp.bfloat16)

    sub = lax.broadcasted_iota(jnp.int32, (nslots, LANES), 0)
    lane = lax.broadcasted_iota(jnp.int32, (nslots, LANES), 1)
    slot_of = sub + rep * nslots
    li, lj = lane // 6, lane % 6
    lo, hi = jnp.minimum(li, lj), jnp.maximum(li, lj)
    entry_of = jnp.where(
        lane < 36, lo * 6 - (lo * (lo - 1)) // 2 + hi - lo,
        jnp.where(lane < 42, lane - 36 + 21, -1),
    )

    def forward(k):
        source = m_send.at[k] if k + 1 == side else m_recv.at[k + rounds]
        return copy_to(source, m_recv.at[k], f_ssem.at[k], m_rsem.at[k], late_of_me, rep)

    @pl.when(is_helper)
    def _():
        pl.semaphore_wait(late_sem, 1)
        for step in order:
            for k in order:
                @pl.when(jnp.logical_and(helps(k + 1), helped(k + 1) == step // 2 + step % 2 * side))
                def _():
                    if k + 1 != side:
                        arrival(k, k + rounds)
                    forward(k).start()

    def returned(k, half):
        return copy_to(
            r_send.at[k], r_recv.at[rep, k], r_ssem.at[half, k], r_rsem.at[rep, k],
            lax.rem(me + k + 1, n_blk), half,
        )

    def turn(step):
        source = jnp.where(me >= n_blk - 2, (step % 2) * side + step // 2, step)
        usual = step * 0
        for place, far in enumerate(far_first):
            usual = jnp.where(step == place, far - 1, usual)
        return jnp.where(is_late, lax.rem(source + n_blk - 1 - me, rounds), usual)

    half = rows // 2
    row_pair = lax.broadcasted_iota(jnp.int32, (half, LANES), 0)
    in_pair = lax.broadcasted_iota(jnp.int32, (2 * LANES, LANES), 0).astype(jnp.float32).astype(jnp.bfloat16)
    one, none = (jnp.full((2 * LANES, LANES), value, jnp.bfloat16) for value in (1.0, 0.0))

    def gather(k):
        arrival(k, k)
        index = m_recv[k, 3].astype(jnp.int32)
        row_of = lax.shift_right_logical(index, 7)
        lane_of = lax.bitwise_and(index, LANES - 1)
        pair_of = lax.shift_right_logical(index, 8)
        spot = lax.bitwise_and(index, 2 * LANES - 1).astype(jnp.float32)
        hot = []
        for j in range(nslots):
            here = jnp.broadcast_to(spot[j : j + 1].astype(jnp.bfloat16), (2 * LANES, LANES))
            hot.append(jnp.where(in_pair == here, one, none))
        chosen = jnp.dot(split[...], jnp.concatenate(hot, axis=1), preferred_element_type=jnp.float32)
        acc = [jnp.zeros((nslots, LANES), jnp.float32)] * 3
        for row in range(rows):
            here = row_of == row
            for c in range(3):
                line = jnp.broadcast_to(tab[0, c, row : row + 1, :], (nslots, LANES))
                got = jnp.take_along_axis(line, lane_of, axis=1, mode="promise_in_bounds")
                acc[c] = jnp.where(here, got, acc[c])
        for j in range(nslots):
            here = row_pair == jnp.broadcast_to(pair_of[j : j + 1], (half, LANES))
            for c in range(3):
                block = chosen[c * rows : (c + 1) * rows, j * LANES : (j + 1) * LANES]
                found = jnp.where(here, block[:half] + block[half:], 0.0)
                found = sum(found[i : i + 8] for i in range(8, half, 8)) + found[:8]
                stage[pl.ds((c * nslots + j) * 8, 8), :] = found
        for c in range(3):
            total = stage[pl.ds(c * nslots * 8, nslots, stride=8), :]
            for i in range(1, 8):
                total = total + stage[pl.ds(c * nslots * 8 + i, nslots, stride=8), :]
            acc.append(total)
        return tuple(acc)

    def gram(k, picked):
        q0, q1, q2, n0, n1, n2 = picked
        live = (slot_of < m_recv[k, 4].astype(jnp.int32)).astype(jnp.float32)
        p0, p1, p2 = m_recv[k, 0], m_recv[k, 1], m_recv[k, 2]
        resid = n0 * (p0 - q0) + n1 * (p1 - q1) + n2 * (p2 - q2)
        weight = live / (1.0 + resid * resid)
        jacob = [p1 * n2 - p2 * n1, p2 * n0 - p0 * n2, p0 * n1 - p1 * n0, n0, n1, n2]
        scaled = [weight * entry for entry in jacob]
        for e, (i, j) in enumerate(ENTRIES):
            prods[pl.ds(e * 8, 8), :] = scaled[i] * jacob[j]
        for i in range(6):
            prods[pl.ds((21 + i) * 8, 8), :] = scaled[i] * resid
        parts = []
        for g in range(4):
            some = prods[pl.ds(g * 64, 8, stride=8), :]
            for t in range(1, 8):
                some = some + prods[pl.ds(g * 64 + t, 8, stride=8), :]
            parts.append(some)
        whole = jnp.dot(
            jnp.concatenate(parts, axis=0), jnp.ones((LANES, LANES), jnp.float32),
            precision=lax.Precision.HIGHEST, preferred_element_type=jnp.float32,
        )
        spread = jnp.zeros((8, LANES), jnp.float32)
        for g in range(4):
            spread = spread + jnp.where(entry_of == sub + g * 8, whole[g * 8 : g * 8 + 8], 0.0)
        line = jnp.sum(spread, axis=0, keepdims=True)
        r_send[k] = line
        return line

    def give_back(k):
        for half in range(2):
            returned(k, half).start()

    def one_step(step, carry):
        picked, tsum = carry[:6], carry[6]
        before, k = turn(step - 1), turn(step)
        arrived = gather(k)
        line = gram(before, picked)
        give_back(before)
        return arrived + (tsum + line,)

    opening = gram(turn(0), gather(turn(0)))
    give_back(turn(0))
    carry = lax.fori_loop(2, rounds, one_step, gather(turn(1)) + (opening,))
    last = turn(rounds - 1)
    line = gram(last, carry[:6])
    give_back(last)
    t_send[...] = carry[6] + line

    exchange = copy_to(t_send, t_recv, t_ssem, t_rsem, me, 1 - rep)
    exchange.start()

    source_sum = jnp.zeros((1, LANES), jnp.float32)
    for k in order:
        for half in range(2):
            copy_to(
                r_send.at[k], r_recv.at[half, k], r_ssem.at[half, k], r_rsem.at[half, k], host(k + 1), half
            ).wait_recv()
        both = r_recv[0, k] + r_recv[1, k]
        out_ref[pl.ds(k, 1), :] = both
        source_sum = source_sum + both
    exchange.wait_recv()
    target_sum = t_send[...] + t_recv[...]
    lane1 = lax.broadcasted_iota(jnp.int32, (1, LANES), 1)
    out_ref[pl.ds(rounds, 1), :] = source_sum + jnp.where(lane1 < 36, target_sum, -target_sum)

    for k in order:
        @pl.when(jnp.logical_not(jnp.logical_and(is_own, k + 1 == side)))
        def _():
            outbound(k).wait_send()

    for k in order:
        for half in range(2):
            returned(k, half).wait_send()
    exchange.wait_send()

    @pl.when(is_helper)
    def _():
        for k in order:
            @pl.when(helps(k + 1))
            def _():
                forward(k).wait_send()


def finish(rounds, total_slots, sums_ref, diag_ref, grad_ref, pair_ref):
    pair_ref[...] = sums_ref[:rounds, :36] * (1.0 / total_slots)
    total = sums_ref[rounds : rounds + 1] * (1.0 / (total_slots * 2.0 * rounds))
    diag_ref[...] = total[:, :36]
    grad_ref[...] = total[:, 36:42]


def solution(mesh):
    n_blk = mesh.shape["blk"]

    def body(points, normals, src_block, tgt_index, active):
        npts = points.shape[2]
        rounds, nslots = src_block.shape[0], src_block.shape[3]
        rows = npts // LANES
        f32, i32 = jnp.float32, jnp.int32
        dma = pltpu.SemaphoreType.DMA
        total_slots = 2 * nslots * LANES
        sums = pl.pallas_call(
            functools.partial(kernel, n_blk, rounds, nslots, npts, SIDE),
            out_shape=jax.ShapeDtypeStruct((rounds + 8, LANES), f32),
            in_specs=[pl.BlockSpec(memory_space=pl.ANY)] * 5,
            out_specs=pl.BlockSpec(memory_space=pltpu.VMEM),
            scratch_shapes=[
                pltpu.VMEM((2, 3, rows, LANES), f32),
                pltpu.VMEM((rounds, nslots, LANES), i32),
                pltpu.SMEM((rounds, nslots), i32),
                pltpu.SMEM((1, rounds), i32),
                pltpu.VMEM((rounds, 5, nslots, LANES), f32),
                pltpu.VMEM((2 * rounds, 5, nslots, LANES), f32),
                pltpu.VMEM((3 * rows, 2 * LANES), jnp.bfloat16),
                pltpu.VMEM((3 * nslots * 8, LANES), f32),
                pltpu.VMEM((256, LANES), f32),
                pltpu.VMEM((rounds, 1, LANES), f32),
                pltpu.VMEM((2, rounds, 1, LANES), f32),
                pltpu.VMEM((1, LANES), f32),
                pltpu.VMEM((1, LANES), f32),
                dma((5,)),
                dma((rounds,)), dma((2 * rounds,)),
                dma((2, rounds)), dma((2, rounds)),
                dma, dma, dma((rounds,)), pltpu.SemaphoreType.REGULAR,
            ],
            compiler_params=pltpu.CompilerParams(collective_id=0, has_side_effects=True, vmem_limit_bytes=8 * 1024 * 1024),
        )(
            pltpu.with_memory_space_constraint(points.reshape(3, rows, LANES), pltpu.HBM),
            pltpu.with_memory_space_constraint(normals.reshape(3, rows, LANES), pltpu.HBM),
            pltpu.with_memory_space_constraint(src_block.reshape(rounds, nslots), pltpu.HBM),
            pltpu.with_memory_space_constraint(tgt_index.reshape(rounds, nslots, LANES), pltpu.HBM),
            pltpu.with_memory_space_constraint(active.reshape(1, rounds), pltpu.HBM),
        )
        diag, grad, pair = pl.pallas_call(
            functools.partial(finish, rounds, total_slots),
            out_shape=(
                jax.ShapeDtypeStruct((1, 36), f32),
                jax.ShapeDtypeStruct((1, 6), f32),
                jax.ShapeDtypeStruct((rounds, 36), f32),
            ),
            compiler_params=pltpu.CompilerParams(vmem_limit_bytes=1024 * 1024),
        )(sums)
        return diag, grad, pair.reshape(rounds, 1, 1, 36)

    return jax.shard_map(
        body,
        mesh=mesh,
        in_specs=(
            P("blk", None, None),
            P("blk", None, None),
            P(None, "blk", None, "rep"),
            P(None, "blk", None, "rep", None),
            P(None, "blk", None),
        ),
        out_specs=(P("blk", None), P("blk", None), P(None, "blk", None, None)),
        check_vma=False,
    )
```
